256 devices in a mesh: copy: 2 (over core), fsdp: 32 (over z, y), tp: 4 (over x).
Axes of the slice: x: 4, y: 4, z: 8, core: 2. Of those that a mesh axis runs over, the one named last changes fastest.
Arguments:
- gradients: float32 [256, 128, 4096], P('copy', 'fsdp', 'tp'), parts along dimension 0, may hold values from -6 to 6
- momentum: float32 [256, 128, 4096], P('copy', 'fsdp', 'tp'), parts along dimension 0, may hold values from -6 to 6
- weights: float32 [256, 128, 4096], P('copy', 'fsdp', 'tp'), parts along dimension 0, may hold values from -0.1875 to 0.1875
Outputs:
- new_weights: float32 [256, 128, 4096], P('copy', 'fsdp', 'tp'), parts along dimension 0
- new_momentum: float32 [256, 128, 4096], P('copy', 'fsdp', 'tp'), parts along dimension 0
The draws below stay inside these ranges and needn't reach their ends.
There are 2 independent parts, one for each index of `copy`. The reference program is written for one: setup_inputs(seed, part) draws one part's arguments, and reference() takes and returns one part's arrays. A program takes and returns all parts, laid end to end along the dimension named above; each array names one. Nothing has to cross between parts.
All inputs are finite; a program needn't handle non-finite values.
Results may differ from the reference program's by a relative error of at most 0.00014.
Values sent between devices are 32-bit elements; how exact they have to be, the bound alone decides.
A program may use at most 64 MiB of HBM per device.

```python
import jax
import jax.numpy as jnp
from jax import lax

SIDE = 128
WIDE = 4096
MATS = 128
ITERS = 4


def steps_of(stream_key, dims, cuts, low, largest):
    gain, own = 1.0, jax.random.fold_in(stream_key, 6)
    for position, shards_of in cuts:
        steps = jnp.exp(jax.random.uniform(jax.random.fold_in(own, position), (shards_of,), jnp.float32, low / len(cuts), largest / len(cuts)))
        gain = gain * jnp.repeat(steps, dims[position] // shards_of).reshape([-1 if axis == position else 1 for axis in range(len(dims))])
    return gain


def normal_values(key, shape, deviation, reach, shards=(), held_as=jnp.bfloat16):
    factor_of = steps_of(key, shape, shards, -0.22, 0.18) if shards else 1.0
    values = jax.random.normal(key, shape, jnp.float32) * deviation * factor_of
    return jnp.minimum(jnp.maximum(values, -reach), reach).astype(held_as)


def setup_inputs(seed: int = 0, part: int = 0) -> dict:
    arg_keys = jax.random.split(jax.random.key(seed), 4)
    own_keys = jax.random.split(jax.random.fold_in(arg_keys[3], part), 4)
    gradients = normal_values(own_keys[0], (MATS, SIDE, WIDE), 1.0, 6.0, ((1, 32), (2, 4)), jnp.float32)
    momentum = normal_values(own_keys[1], (MATS, SIDE, WIDE), 1.0, 6.0, ((1, 32), (2, 4)), jnp.float32)
    weights = normal_values(own_keys[2], (MATS, SIDE, WIDE), 0.03, 0.1875, ((1, 32), (2, 4)), jnp.float32)
    return dict(gradients=gradients, momentum=momentum, weights=weights)


hold_rate = 0.95
learn_rate = 0.9
decay_rate = 0.1

def reference(gradients, momentum, weights):
    new_momentum = hold_rate * momentum + gradients
    direction = hold_rate * new_momentum + gradients

    def orthogonal_one(stack):
        iterate = stack[None]
        iterate = iterate * lax.rsqrt(lax.optimization_barrier(jnp.sum(iterate * iterate, axis=(1, 2), keepdims=True)) + 1e-06)
        for step in range(ITERS):
            gram = jnp.einsum('mik,mjk->mij', iterate, iterate, precision=lax.Precision.HIGHEST)
            mixed = -4.775 * gram + 2.0315 * jnp.einsum('mij,mjk->mik', gram, gram, precision=lax.Precision.HIGHEST)
            iterate = 3.4445 * iterate + jnp.einsum('mij,mjk->mik', mixed, iterate, precision=lax.Precision.HIGHEST)
        return iterate[0]
    iterate = lax.map(orthogonal_one, direction)
    new_weights = (1.0 - learn_rate * decay_rate) * weights - learn_rate * iterate
    return (new_weights, new_momentum)
```

```python
import jax
import jax.numpy as jnp
from jax import lax
from jax.sharding import PartitionSpec as P

ITERS = 4


hold_rate = 0.95
learn_rate = 0.9
decay_rate = 0.1


def product(a, b):
    return jnp.einsum("mij,mjk->mik", a, b, precision=lax.Precision.HIGHEST)


def sent_to_all(x, axis):
    length = lax.axis_size(axis)
    return lax.all_to_all(jnp.broadcast_to(x[None], (length, *x.shape)), axis, 0, 0, tiled=True)


def shards(gradients, momentum, weights):
    new_momentum = hold_rate * momentum + gradients
    direction = hold_rate * new_momentum + gradients
    moved = lax.all_to_all(direction, "fsdp", split_axis=0, concat_axis=1, tiled=True)
    gram = sent_to_all(
        jnp.einsum("mik,mjk->mij", moved, moved, precision=lax.Precision.HIGHEST), "tp"
    ).sum(axis=0)
    eye = jnp.eye(gram.shape[-1], dtype=gram.dtype)
    total = jnp.sum(gram * eye, axis=(1, 2), keepdims=True)
    scale = lax.rsqrt(total + 1e-06)
    gram = gram * (scale * scale)
    taken = None
    for step in range(ITERS):
        mixed = 3.4445 * eye - 4.775 * gram + 2.0315 * product(gram, gram)
        taken = mixed if taken is None else product(mixed, taken)
        if step < ITERS - 1:
            gram = product(product(mixed, gram), mixed)
    iterate = product(taken * scale, moved)
    back = lax.all_to_all(iterate, "fsdp", split_axis=1, concat_axis=0, tiled=True)
    new_weights = (1.0 - learn_rate * decay_rate) * weights - learn_rate * back
    return (new_weights, new_momentum)


def solution(mesh):
    return jax.shard_map(
        shards,
        mesh=mesh,
        in_specs=(P("copy", "fsdp", "tp"), P("copy", "fsdp", "tp"), P("copy", "fsdp", "tp")),
        out_specs=(P("copy", "fsdp", "tp"), P("copy", "fsdp", "tp")),
        check_vma=False,
    )
```

```python
import jax
import jax.numpy as jnp
from jax import lax
from jax.experimental import pallas as pl
from jax.experimental.pallas import tpu as pltpu
from jax.sharding import PartitionSpec as P

ITERS = 4


hold_rate = 0.95
learn_rate = 0.9
decay_rate = 0.1

MESH = pl.DeviceIdType.MESH
HIGHEST = lax.Precision.HIGHEST


def dot(a, b, contract=((1,), (0,))):
    return lax.dot_general(
        a, b, (contract, ((), ())), precision=HIGHEST, preferred_element_type=jnp.float32
    )


def partner(me, i):
    j = i // 4
    dz = lax.rem(8 + (2 * lax.rem(j, 2) - 1) * ((j + 1) // 2), 8)
    z = lax.rem(me // 4 + dz, 8)
    y = lax.rem(lax.rem(me, 4) + lax.rem(i, 4), 4)
    return z * 4 + y


def swapped(a, b):
    upper = lax.broadcasted_iota(jnp.int32, a.shape, 0) < 4
    return (
        jnp.where(upper, a, pltpu.roll(b, 4, 0)),
        jnp.where(upper, pltpu.roll(a, 4, 0), b),
    )


def kernel(
    g_hbm, m_hbm, w_hbm, new_w_hbm, new_m_hbm,
    g, m, w, new_m, out, away, there, home, back, mats, gram, grams,
    load_sem, w_sem, store_sem, w_out_sem, away_send, away_recv, home_send, home_recv, gram_send, gram_recv,
):
    fsdp = lax.axis_size("fsdp")
    tp = lax.axis_size("tp")
    me = lax.axis_index("fsdp")
    col = lax.axis_index("tp")

    barrier = pltpu.get_barrier_semaphore()

    @pl.loop(1, fsdp)
    def _(i):
        pl.semaphore_signal(barrier, inc=1, device_id={"fsdp": partner(me, i)}, device_id_type=MESH)

    @pl.loop(1, tp)
    def _(i):
        pl.semaphore_signal(
            barrier, inc=1, device_id={"tp": lax.rem(col + i, tp)}, device_id_type=MESH
        )

    load_g = pltpu.make_async_copy(g_hbm, g, load_sem.at[0])
    load_m = pltpu.make_async_copy(m_hbm, m, load_sem.at[1])
    load_w = pltpu.make_async_copy(w_hbm, w, w_sem)
    load_g.start()
    load_m.start()
    load_w.start()
    load_g.wait()
    load_m.wait()

    @pl.loop(0, fsdp)
    def _(d):
        for k in range(4):
            grad = g[d, k]
            momentum = hold_rate * m[d, k] + grad
            new_m[d, k] = momentum
            away[k // 2, d, pl.ds(4 * (k % 2), 4), :] = hold_rate * momentum + grad

    store_m = pltpu.make_async_copy(new_m, new_m_hbm, store_sem)
    store_m.start()
    pl.semaphore_wait(barrier, fsdp - 1 + tp - 1)

    for c in range(2):
        @pl.loop(1, fsdp)
        def _(i):
            d = partner(me, i)
            pltpu.make_async_remote_copy(
                src_ref=away.at[c, d],
                dst_ref=there.at[c, me],
                send_sem=away_send.at[c],
                recv_sem=away_recv.at[c],
                device_id={"fsdp": d},
                device_id_type=MESH,
            ).start()

        there[c, me] = away[c, me]

    for c in range(2):
        others = there.at[c, pl.ds(0, fsdp - 1)]
        pltpu.make_async_copy(others, others, away_recv.at[c]).wait()

        @pl.loop(0, fsdp // 2)
        def _(j):
            first, second = swapped(there[c, 2 * j], there[c, 2 * j + 1])
            rows = pl.ds(pl.multiple_of(8 * j, 8), 8)
            mats[0, rows, :] = first
            mats[1, rows, :] = second

        for k in range(2):
            x = mats[k]
            gram[c, k] = dot(x, x, ((1,), (1,)))

        @pl.loop(1, tp)
        def _(i):
            pltpu.make_async_remote_copy(
                src_ref=gram.at[c],
                dst_ref=grams.at[c, col],
                send_sem=gram_send.at[c],
                recv_sem=gram_recv.at[c],
                device_id={"tp": lax.rem(col + i, tp)},
                device_id_type=MESH,
            ).start()

        grams[c, col] = gram[c]
        others = grams.at[c, pl.ds(0, tp - 1)]
        pltpu.make_async_copy(others, others, gram_recv.at[c]).wait()

        shape = gram.shape[2:]
        eye = (
            lax.broadcasted_iota(jnp.int32, shape, 0) == lax.broadcasted_iota(jnp.int32, shape, 1)
        ).astype(jnp.float32)
        takens = []
        for k in range(2):
            a = (grams[c, 0, k] + grams[c, 1, k]) + (grams[c, 2, k] + grams[c, 3, k])
            total = jnp.sum(jnp.sum(a * eye, axis=1, keepdims=True), axis=0, keepdims=True)
            scale = lax.rsqrt(total + 1e-06)
            a = a * (scale * scale)
            taken = None
            for step in range(ITERS):
                mixed = 3.4445 * eye - 4.775 * a + 2.0315 * dot(a, a)
                taken = mixed if taken is None else dot(mixed, taken)
                if step < ITERS - 1:
                    a = dot(dot(mixed, a), mixed)
            takens.append(taken * scale)
        for k in range(2):
            mats[k] = dot(takens[k], mats[k])

        @pl.loop(0, fsdp // 2)
        def _(j):
            rows = pl.ds(pl.multiple_of(8 * j, 8), 8)
            first, second = swapped(mats[0, rows, :], mats[1, rows, :])
            home[c, 2 * j] = first
            home[c, 2 * j + 1] = second

        @pl.loop(1, fsdp)
        def _(i):
            d = partner(me, i)
            pltpu.make_async_remote_copy(
                src_ref=home.at[c, d],
                dst_ref=back.at[c, me],
                send_sem=home_send.at[c],
                recv_sem=home_recv.at[c],
                device_id={"fsdp": d},
                device_id_type=MESH,
            ).start()

        back[c, me] = home[c, me]

    load_w.wait()
    for c in range(2):
        others = back.at[c, pl.ds(0, fsdp - 1)]
        pltpu.make_async_copy(others, others, home_recv.at[c]).wait()

        @pl.loop(0, fsdp)
        def _(d):
            for k in range(2):
                out[d, 2 * c + k] = (1.0 - learn_rate * decay_rate) * w[d, 2 * c + k] - learn_rate * back[
                    c, d, pl.ds(4 * k, 4), :
                ]

        pltpu.make_async_copy(
            out.at[:, pl.ds(2 * c, 2)], new_w_hbm.at[:, pl.ds(2 * c, 2)], w_out_sem.at[c]
        ).start()

    for c in range(2):
        pltpu.make_async_copy(
            out.at[:, pl.ds(2 * c, 2)], new_w_hbm.at[:, pl.ds(2 * c, 2)], w_out_sem.at[c]
        ).wait()
        sent = away.at[c, pl.ds(0, fsdp - 1)]
        pltpu.make_async_copy(sent, sent, away_send.at[c]).wait()
        pltpu.make_async_copy(sent, sent, home_send.at[c]).wait()
        sent = grams.at[c, pl.ds(0, tp - 1)]
        pltpu.make_async_copy(sent, sent, gram_send.at[c]).wait()
    store_m.wait()


def shards(gradients, momentum, weights):
    mats, side, wide = gradients.shape
    fsdp = lax.axis_size("fsdp")
    tp = lax.axis_size("tp")
    shape = (fsdp, mats // fsdp, side, wide)
    rows = side * fsdp
    f32 = jnp.float32
    block = pltpu.VMEM(shape, f32)
    tiles = pltpu.VMEM((2, fsdp, 2 * side, wide), f32)
    sem = pltpu.SemaphoreType.DMA
    new_weights, new_momentum = pl.pallas_call(
        kernel,
        out_shape=[jax.ShapeDtypeStruct(shape, f32)] * 2,
        in_specs=[pl.BlockSpec(memory_space=pl.ANY)] * 3,
        out_specs=[pl.BlockSpec(memory_space=pl.ANY)] * 2,
        scratch_shapes=[
            block, block, block, block, block, tiles, tiles, tiles, tiles,
            pltpu.VMEM((2, rows, wide), f32),
            pltpu.VMEM((2, 2, rows, rows), f32),
            pltpu.VMEM((2, tp, 2, rows, rows), f32),
            sem((2,)), sem, sem, sem((2,)), sem((2,)), sem((2,)), sem((2,)), sem((2,)), sem((2,)), sem((2,)),
        ],
        compiler_params=pltpu.CompilerParams(
            collective_id=0, has_side_effects=True, vmem_limit_bytes=48 * 1024 * 1024
        ),
        name="update",
    )(gradients.reshape(shape), momentum.reshape(shape), weights.reshape(shape))
    return new_weights.reshape(gradients.shape), new_momentum.reshape(gradients.shape)


def solution(mesh):
    return jax.shard_map(
        shards,
        mesh=mesh,
        in_specs=(P("copy", "fsdp", "tp"), P("copy", "fsdp", "tp"), P("copy", "fsdp", "tp")),
        out_specs=(P("copy", "fsdp", "tp"), P("copy", "fsdp", "tp")),
        check_vma=False,
    )
```

```python
import jax
import jax.numpy as jnp
from jax import lax
from jax.experimental import pallas as pl
from jax.experimental.pallas import tpu as pltpu
from jax.sharding import PartitionSpec as P

ITERS = 4


hold_rate = 0.95
learn_rate = 0.9
decay_rate = 0.1

ZS, YS = 8, 4
OUTWARD = (1, 7, 0, 2, 6, 3, 5, 4)
MESH = pl.DeviceIdType.MESH
HIGHEST = lax.Precision.HIGHEST


def dot(a, b, contract=((1,), (0,))):
    return lax.dot_general(
        a, b, (contract, ((), ())), precision=HIGHEST, preferred_element_type=jnp.float32
    )


def send(src, dst, send_sem, recv_sem, device):
    pltpu.make_async_remote_copy(
        src_ref=src, dst_ref=dst, send_sem=send_sem, recv_sem=recv_sem, device_id=device, device_id_type=MESH
    ).start()


def wait(ref, sem):
    pltpu.make_async_copy(ref, ref, sem).wait()


def swapped(a, b):
    upper = lax.broadcasted_iota(jnp.int32, a.shape, 0) < 4
    return (
        jnp.where(upper, a, pltpu.roll(b, 4, 0)),
        jnp.where(upper, pltpu.roll(a, 4, 0), b),
    )


def iterated(grams):
    shape = grams[0].shape
    eye = (
        lax.broadcasted_iota(jnp.int32, shape, 0) == lax.broadcasted_iota(jnp.int32, shape, 1)
    ).astype(jnp.float32)
    scales = [
        lax.rsqrt(jnp.sum(jnp.sum(a * eye, axis=1, keepdims=True), axis=0, keepdims=True) + 1e-06)
        for a in grams
    ]
    grams = [a * (scale * scale) for a, scale in zip(grams, scales)]
    takens = None
    for step in range(ITERS):
        mixed = [3.4445 * eye - 4.775 * a + 2.0315 * dot(a, a) for a in grams]
        if step < ITERS - 1:
            halves = [dot(m, a) for m, a in zip(mixed, grams)]
        takens = mixed if takens is None else [dot(m, t) for m, t in zip(mixed, takens)]
        if step < ITERS - 1:
            grams = [dot(h, m) for h, m in zip(halves, mixed)]
    return [t * scale for t, scale in zip(takens, scales)]


def kernel(
    g_hbm, m_hbm, w_hbm, new_w, new_m,
    g, m, w, away, there, home, back, mats, gram, grams,
    load_sem, w_sem, away_send, away_recv, home_send, home_recv, gram_send, gram_recv, ready,
):
    fsdp = lax.axis_size("fsdp")
    tp = lax.axis_size("tp")
    me = lax.axis_index("fsdp")
    col = lax.axis_index("tp")
    core = lax.axis_index("copy")
    own_y = lax.rem(me, YS)
    planes = [lax.rem(me // YS + k, ZS) * YS for k in range(ZS)]
    ys = [lax.rem(own_y + k, YS) for k in range(YS)]
    shifted = [lax.rem(own_y + core + k, YS) for k in range(YS)]

    def partners(dz):
        if dz == 0:
            return [planes[0] + ys[k] for k in range(1, YS)]
        return [planes[dz] + shifted[(k + (2 if dz > ZS // 2 else 0)) % YS] for k in range(YS)]

    def load(dz):
        rows = pl.ds(planes[dz], YS)
        return [
            pltpu.make_async_copy(x.at[rows], y.at[rows], load_sem.at[dz, n])
            for n, (x, y) in enumerate(((g_hbm, g), (m_hbm, m)))
        ]

    def direct(dz):
        for copy in load(dz):
            copy.wait()

        @pl.loop(0, YS)
        def _(y):
            d = planes[dz] + y
            for k in range(4):
                grad = g[d, k]
                momentum = hold_rate * m[d, k] + grad
                new_m[d, k] = momentum
                away[k // 2, d, pl.ds(4 * (k % 2), 4), :] = hold_rate * momentum + grad

    def send_away(c, dz):
        for d in partners(dz):
            send(away.at[c, d], there.at[c, me], away_send.at[c], away_recv.at[c], {"fsdp": d})

    def tell(n):
        for dz in (1, ZS - 1):
            pl.semaphore_signal(
                ready.at[n], inc=1, device_id={"fsdp": planes[dz] + own_y}, device_id_type=MESH
            )

    barrier = pltpu.get_barrier_semaphore()
    for dz in (1, ZS - 1, 0):
        for k in range(YS):
            if dz or k:
                pl.semaphore_signal(
                    barrier, inc=1, device_id={"fsdp": planes[dz] + ys[k]}, device_id_type=MESH
                )
    for k in range(1, 4):
        pl.semaphore_signal(barrier, inc=1, device_id={"tp": lax.rem(col + k, tp)}, device_id_type=MESH)

    for dz in OUTWARD:
        for copy in load(dz):
            copy.start()
    for dz in (1, ZS - 1, 0):
        direct(dz)

    pl.semaphore_wait(barrier, 3 * YS - 1 + tp - 1)
    tell(0)
    for c in range(2):
        for dz in (1, ZS - 1):
            send_away(c, dz)
        if c == 0:
            send_away(c, 0)
    for n in range(2):
        for dz in (n + 2, ZS - 2 - n):
            direct(dz)
        pl.semaphore_wait(ready.at[n], 2)
        tell(n + 1)
        for dz in (n + 2, ZS - 2 - n):
            send_away(0, dz)
    direct(4)
    pl.semaphore_wait(ready.at[2], 2)
    send_away(0, 4)
    for dz in (4, 5, 3, 6, 2, 0):
        send_away(1, dz)
    load_w = pltpu.make_async_copy(w_hbm, w, w_sem)
    load_w.start()
    for c in range(2):
        there[c, me] = away[c, me]

    @pl.loop(0, 2)
    def _(c):
        wait(there.at[c, pl.ds(0, fsdp - 1)], away_recv.at[c])

        @pl.loop(0, fsdp // 2)
        def _(j):
            first, second = swapped(there[c, 2 * j], there[c, 2 * j + 1])
            rows = pl.ds(pl.multiple_of(8 * j, 8), 8)
            mats[0, rows, :] = first
            mats[1, rows, :] = second

        for k in range(2):
            x = mats[k]
            gram[c, k] = dot(x, x, ((1,), (1,)))
        for k in range(1, 4):
            send(gram.at[c], grams.at[c, col], gram_send.at[c], gram_recv.at[c], {"tp": lax.rem(col + k, tp)})
        grams[c, col] = gram[c]
        wait(grams.at[c, pl.ds(0, tp - 1)], gram_recv.at[c])

        takens = iterated(
            [(grams[c, 0, k] + grams[c, 1, k]) + (grams[c, 2, k] + grams[c, 3, k]) for k in range(2)]
        )
        for k in range(2):
            mats[k] = dot(takens[k], mats[k])

        @pl.loop(0, fsdp // 2)
        def _(j):
            rows = pl.ds(pl.multiple_of(8 * j, 8), 8)
            first, second = swapped(mats[0, rows, :], mats[1, rows, :])
            home[c, 2 * j] = first
            home[c, 2 * j + 1] = second

        for dz in (0, 4, 5, 3, 6, 2, 7, 1):
            for d in partners(dz):
                send(home.at[c, d], back.at[c, me], home_send.at[c], home_recv.at[c], {"fsdp": d})
        back[c, me] = home[c, me]

    load_w.wait()
    for c in range(2):
        wait(back.at[c, pl.ds(0, fsdp - 1)], home_recv.at[c])

        @pl.loop(0, fsdp)
        def _(d):
            for k in range(2):
                new_w[d, 2 * c + k] = (1.0 - learn_rate * decay_rate) * w[d, 2 * c + k] - learn_rate * back[
                    c, d, pl.ds(4 * k, 4), :
                ]

    for c in range(2):
        wait(away.at[c, pl.ds(0, fsdp - 1)], away_send.at[c])
        wait(home.at[c, pl.ds(0, fsdp - 1)], home_send.at[c])
        wait(grams.at[c, pl.ds(0, tp - 1)], gram_send.at[c])


def shards(gradients, momentum, weights):
    mats, side, wide = gradients.shape
    fsdp = lax.axis_size("fsdp")
    tp = lax.axis_size("tp")
    shape = (fsdp, mats // fsdp, side, wide)
    rows = side * fsdp
    f32 = jnp.float32
    block = pltpu.VMEM(shape, f32)
    tiles = pltpu.VMEM((2, fsdp, 2 * side, wide), f32)
    sem = pltpu.SemaphoreType.DMA
    new_weights, new_momentum = pl.pallas_call(
        kernel,
        out_shape=[jax.ShapeDtypeStruct(shape, f32)] * 2,
        in_specs=[pl.BlockSpec(memory_space=pl.ANY)] * 3,
        out_specs=[pl.BlockSpec(memory_space=pltpu.VMEM)] * 2,
        scratch_shapes=[
            block, block, block, tiles, tiles, tiles, tiles,
            pltpu.VMEM((2, rows, wide), f32),
            pltpu.VMEM((2, 2, rows, rows), f32),
            pltpu.VMEM((2, tp, 2, rows, rows), f32),
            sem((ZS, 2)), sem, sem((2,)), sem((2,)), sem((2,)), sem((2,)), sem((2,)), sem((2,)),
            pltpu.SemaphoreType.REGULAR((3,)),
        ],
        compiler_params=pltpu.CompilerParams(
            collective_id=0, has_side_effects=True, vmem_limit_bytes=48 * 1024 * 1024
        ),
        name="update",
    )(gradients.reshape(shape), momentum.reshape(shape), weights.reshape(shape))
    return new_weights.reshape(gradients.shape), new_momentum.reshape(gradients.shape)


def solution(mesh):
    return jax.shard_map(
        shards,
        mesh=mesh,
        in_specs=(P("copy", "fsdp", "tp"), P("copy", "fsdp", "tp"), P("copy", "fsdp", "tp")),
        out_specs=(P("copy", "fsdp", "tp"), P("copy", "fsdp", "tp")),
        check_vma=False,
    )
```

```python
import jax
import jax.numpy as jnp
from jax import lax
from jax.experimental import pallas as pl
from jax.experimental.pallas import tpu as pltpu
from jax.sharding import PartitionSpec as P

ITERS = 4


hold_rate = 0.95
learn_rate = 0.9
decay_rate = 0.1

ZS, YS = 8, 4
OUTWARD = (1, 7, 0, 2, 6, 3, 5, 4)
MESH = pl.DeviceIdType.MESH
HIGHEST = lax.Precision.HIGHEST


def dot(a, b, contract=((1,), (0,))):
    return lax.dot_general(
        a, b, (contract, ((), ())), precision=HIGHEST, preferred_element_type=jnp.float32
    )


def send(src, dst, send_sem, recv_sem, device):
    pltpu.make_async_remote_copy(
        src_ref=src, dst_ref=dst, send_sem=send_sem, recv_sem=recv_sem, device_id=device, device_id_type=MESH
    ).start()


def wait(ref, sem):
    pltpu.make_async_copy(ref, ref, sem).wait()


def swapped(a, b):
    upper = lax.broadcasted_iota(jnp.int32, a.shape, 0) < 4
    return (
        jnp.where(upper, a, pltpu.roll(b, 4, 0)),
        jnp.where(upper, pltpu.roll(a, 4, 0), b),
    )


def iterated(grams):
    shape = grams[0].shape
    eye = (
        lax.broadcasted_iota(jnp.int32, shape, 0) == lax.broadcasted_iota(jnp.int32, shape, 1)
    ).astype(jnp.float32)
    scales = [
        lax.rsqrt(jnp.sum(jnp.sum(a * eye, axis=1, keepdims=True), axis=0, keepdims=True) + 1e-06)
        for a in grams
    ]
    grams = [a * (scale * scale) for a, scale in zip(grams, scales)]
    takens = None
    for step in range(ITERS):
        mixed = [3.4445 * eye - 4.775 * a + 2.0315 * dot(a, a) for a in grams]
        if step < ITERS - 1:
            halves = [dot(m, a) for m, a in zip(mixed, grams)]
        takens = mixed if takens is None else [dot(m, t) for m, t in zip(mixed, takens)]
        if step < ITERS - 1:
            grams = [dot(h, m) for h, m in zip(halves, mixed)]
    return [t * scale for t, scale in zip(takens, scales)]


def kernel(
    g_hbm, m_hbm, w_hbm, new_w, new_m,
    g, m, w, away, there, home, back, mats, gram, grams,
    load_sem, w_sem, away_send, away_recv, home_send, home_recv, gram_send, gram_recv, ready,
):
    fsdp = lax.axis_size("fsdp")
    tp = lax.axis_size("tp")
    me = lax.axis_index("fsdp")
    col = lax.axis_index("tp")
    core = lax.axis_index("copy")
    own_y = lax.rem(me, YS)
    planes = [lax.rem(me // YS + k, ZS) * YS for k in range(ZS)]
    ys = [lax.rem(own_y + k, YS) for k in range(YS)]
    shifted = [lax.rem(own_y + core + k, YS) for k in range(YS)]

    def partners(dz):
        if dz == 0:
            return [planes[0] + ys[k] for k in range(1, YS)]
        return [planes[dz] + shifted[(k + (2 if dz > ZS // 2 else 0)) % YS] for k in range(YS)]

    def load(dz):
        rows = pl.ds(planes[dz], YS)
        return [
            pltpu.make_async_copy(x.at[rows], y.at[rows], load_sem.at[dz, n])
            for n, (x, y) in enumerate(((g_hbm, g), (m_hbm, m)))
        ]

    def direct(dz):
        for copy in load(dz):
            copy.wait()

        @pl.loop(0, YS)
        def _(y):
            d = planes[dz] + y
            for k in range(4):
                grad = g[d, k]
                momentum = hold_rate * m[d, k] + grad
                new_m[d, k] = momentum
                away[k // 2, d, pl.ds(4 * (k % 2), 4), :] = hold_rate * momentum + grad

    def send_away(c, dz):
        for d in partners(dz):
            send(away.at[c, d], there.at[c, me], away_send.at[c], away_recv.at[c], {"fsdp": d})

    def tell(n):
        for dz in (1, ZS - 1):
            pl.semaphore_signal(
                ready.at[n], inc=1, device_id={"fsdp": planes[dz] + own_y}, device_id_type=MESH
            )

    barrier = pltpu.get_barrier_semaphore()
    for dz in (1, ZS - 1, 0):
        for k in range(YS):
            if dz or k:
                pl.semaphore_signal(
                    barrier, inc=1, device_id={"fsdp": planes[dz] + ys[k]}, device_id_type=MESH
                )
    for k in range(1, 4):
        pl.semaphore_signal(barrier, inc=1, device_id={"tp": lax.rem(col + k, tp)}, device_id_type=MESH)

    for dz in OUTWARD:
        for copy in load(dz):
            copy.start()
    for dz in (1, ZS - 1, 0):
        direct(dz)

    pl.semaphore_wait(barrier, 3 * YS - 1 + tp - 1)
    tell(0)
    for c in range(2):
        for dz in (1, ZS - 1):
            send_away(c, dz)
        if c == 0:
            send_away(c, 0)
    for n in range(2):
        for dz in (n + 2, ZS - 2 - n):
            direct(dz)
        pl.semaphore_wait(ready.at[n], 2)
        tell(n + 1)
        for dz in (n + 2, ZS - 2 - n):
            send_away(0, dz)
    direct(4)
    pl.semaphore_wait(ready.at[2], 2)
    send_away(0, 4)
    for dz in (4, 5, 3, 6, 2, 0):
        send_away(1, dz)
    load_w = pltpu.make_async_copy(w_hbm, w, w_sem)
    load_w.start()
    for c in range(2):
        there[c, me] = away[c, me]

    @pl.loop(0, 2)
    def _(c):
        wait(there.at[c, pl.ds(0, fsdp - 1)], away_recv.at[c])

        @pl.loop(0, fsdp // 2)
        def _(j):
            first, second = swapped(there[c, 2 * j], there[c, 2 * j + 1])
            rows = pl.ds(pl.multiple_of(8 * j, 8), 8)
            mats[0, rows, :] = first
            mats[1, rows, :] = second

        for k in range(2):
            x = mats[k]
            gram[c, k] = dot(x, x, ((1,), (1,)))
        for k in range(1, 4):
            send(gram.at[c], grams.at[c, col], gram_send.at[c], gram_recv.at[c], {"tp": lax.rem(col + k, tp)})
        grams[c, col] = gram[c]
        wait(grams.at[c, pl.ds(0, tp - 1)], gram_recv.at[c])

        takens = iterated(
            [(grams[c, 0, k] + grams[c, 1, k]) + (grams[c, 2, k] + grams[c, 3, k]) for k in range(2)]
        )
        for k in range(2):
            mats[k] = dot(takens[k], mats[k])

        @pl.loop(0, fsdp // 2)
        def _(j):
            rows = pl.ds(pl.multiple_of(8 * j, 8), 8)
            first, second = swapped(mats[0, rows, :], mats[1, rows, :])
            home[c, 2 * j] = first
            home[c, 2 * j + 1] = second

        for dz in (0, 4, 5, 3, 6, 2, 7, 1):
            for d in partners(dz):
                send(home.at[c, d], back.at[c, me], home_send.at[c], home_recv.at[c], {"fsdp": d})
        back[c, me] = home[c, me]

    load_w.wait()
    for c in range(2):
        wait(back.at[c, pl.ds(0, fsdp - 1)], home_recv.at[c])

        @pl.loop(0, fsdp)
        def _(d):
            for k in range(2):
                new_w[d, 2 * c + k] = (1.0 - learn_rate * decay_rate) * w[d, 2 * c + k] - learn_rate * back[
                    c, d, pl.ds(4 * k, 4), :
                ]

    for c in range(2):
        wait(away.at[c, pl.ds(0, fsdp - 1)], away_send.at[c])
        wait(home.at[c, pl.ds(0, fsdp - 1)], home_send.at[c])
        wait(grams.at[c, pl.ds(0, tp - 1)], gram_send.at[c])


def stored(a, b, a_out, b_out, sems):
    copies = [
        pltpu.make_async_copy(a, a_out, sems.at[0]),
        pltpu.make_async_copy(b, b_out, sems.at[1]),
    ]
    for copy in copies:
        copy.start()
    for copy in copies:
        copy.wait()


def shards(gradients, momentum, weights):
    mats, side, wide = gradients.shape
    fsdp = lax.axis_size("fsdp")
    tp = lax.axis_size("tp")
    shape = (fsdp, mats // fsdp, side, wide)
    rows = side * fsdp
    f32 = jnp.float32
    block = pltpu.VMEM(shape, f32)
    tiles = pltpu.VMEM((2, fsdp, 2 * side, wide), f32)
    sem = pltpu.SemaphoreType.DMA
    new_weights, new_momentum = pl.pallas_call(
        kernel,
        out_shape=[jax.ShapeDtypeStruct(shape, f32)] * 2,
        in_specs=[pl.BlockSpec(memory_space=pl.ANY)] * 3,
        out_specs=[pl.BlockSpec(memory_space=pltpu.VMEM)] * 2,
        scratch_shapes=[
            block, block, block, tiles, tiles, tiles, tiles,
            pltpu.VMEM((2, rows, wide), f32),
            pltpu.VMEM((2, 2, rows, rows), f32),
            pltpu.VMEM((2, tp, 2, rows, rows), f32),
            sem((ZS, 2)), sem, sem((2,)), sem((2,)), sem((2,)), sem((2,)), sem((2,)), sem((2,)),
            pltpu.SemaphoreType.REGULAR((3,)),
        ],
        compiler_params=pltpu.CompilerParams(
            collective_id=0, has_side_effects=True, vmem_limit_bytes=48 * 1024 * 1024
        ),
        name="update",
    )(gradients.reshape(shape), momentum.reshape(shape), weights.reshape(shape))
    new_weights, new_momentum = pl.pallas_call(
        stored,
        out_shape=[jax.ShapeDtypeStruct(shape, f32)] * 2,
        in_specs=[pl.BlockSpec(memory_space=pl.ANY)] * 2,
        out_specs=[pl.BlockSpec(memory_space=pl.ANY)] * 2,
        scratch_shapes=[sem((2,))],
        compiler_params=pltpu.CompilerParams(vmem_limit_bytes=1024 * 1024),
        name="stored",
    )(new_weights, new_momentum)
    return new_weights.reshape(gradients.shape), new_momentum.reshape(gradients.shape)


def solution(mesh):
    return jax.shard_map(
        shards,
        mesh=mesh,
        in_specs=(P("copy", "fsdp", "tp"), P("copy", "fsdp", "tp"), P("copy", "fsdp", "tp")),
        out_specs=(P("copy", "fsdp", "tp"), P("copy", "fsdp", "tp")),
        check_vma=False,
    )
```

```python
import jax
import jax.numpy as jnp
from jax import lax
from jax.experimental import pallas as pl
from jax.experimental.pallas import tpu as pltpu
from jax.sharding import PartitionSpec as P

ITERS = 4


hold_rate = 0.95
learn_rate = 0.9
decay_rate = 0.1

ZS, YS = 8, 4
OUTWARD = (1, 7, 0, 2, 6, 3, 5, 4)
MESH = pl.DeviceIdType.MESH
HIGHEST = lax.Precision.HIGHEST


def dot(a, b, contract=((1,), (0,))):
    return lax.dot_general(
        a, b, (contract, ((), ())), precision=HIGHEST, preferred_element_type=jnp.float32
    )


def send(src, dst, send_sem, recv_sem, device):
    pltpu.make_async_remote_copy(
        src_ref=src, dst_ref=dst, send_sem=send_sem, recv_sem=recv_sem, device_id=device, device_id_type=MESH
    ).start()


def wait(ref, sem):
    pltpu.make_async_copy(ref, ref, sem).wait()


def swapped(a, b):
    upper = lax.broadcasted_iota(jnp.int32, a.shape, 0) < 4
    return (
        jnp.where(upper, a, pltpu.roll(b, 4, 0)),
        jnp.where(upper, pltpu.roll(a, 4, 0), b),
    )


def iterated(grams):
    shape = grams[0].shape
    eye = (
        lax.broadcasted_iota(jnp.int32, shape, 0) == lax.broadcasted_iota(jnp.int32, shape, 1)
    ).astype(jnp.float32)
    scales = [
        lax.rsqrt(jnp.sum(jnp.sum(a * eye, axis=1, keepdims=True), axis=0, keepdims=True) + 1e-06)
        for a in grams
    ]
    grams = [a * (scale * scale) for a, scale in zip(grams, scales)]
    takens = None
    for step in range(ITERS):
        mixed = [3.4445 * eye - 4.775 * a + 2.0315 * dot(a, a) for a in grams]
        if step < ITERS - 1:
            halves = [dot(m, a) for m, a in zip(mixed, grams)]
        takens = mixed if takens is None else [dot(m, t) for m, t in zip(mixed, takens)]
        if step < ITERS - 1:
            grams = [dot(h, m) for h, m in zip(halves, mixed)]
    return [t * scale for t, scale in zip(takens, scales)]


def kernel(
    g_hbm, m_hbm, w_hbm, new_w, new_m,
    g, m, w, away, there, home, back, mats, gram, grams,
    load_sem, w_sem, away_send, away_recv, home_send, home_recv, gram_send, gram_recv, ready,
):
    fsdp = lax.axis_size("fsdp")
    tp = lax.axis_size("tp")
    me = lax.axis_index("fsdp")
    col = lax.axis_index("tp")
    core = lax.axis_index("copy")
    own_y = lax.rem(me, YS)
    planes = [lax.rem(me // YS + k, ZS) * YS for k in range(ZS)]
    ys = [lax.rem(own_y + k, YS) for k in range(YS)]
    shifted = [lax.rem(own_y + core + k, YS) for k in range(YS)]

    def partners(dz):
        if dz == 0:
            return [planes[0] + ys[k] for k in range(1, YS)]
        return [planes[dz] + shifted[(k + (2 if dz > ZS // 2 else 0)) % YS] for k in range(YS)]

    one, three = lax.rem(own_y + 1 + 2 * core, YS), lax.rem(own_y + 3 - 2 * core, YS)

    def partners_home(dz):
        if dz == 0:
            return partners(0)
        turn = [one, three] if dz <= ZS // 2 else [three, one]
        return [planes[dz] + y for y in (ys[2], *turn, ys[0])]

    def load(dz):
        rows = pl.ds(planes[dz], YS)
        return [
            pltpu.make_async_copy(x.at[rows], y.at[rows], load_sem.at[dz, n])
            for n, (x, y) in enumerate(((g_hbm, g), (m_hbm, m)))
        ]

    def direct(dz):
        for copy in load(dz):
            copy.wait()

        @pl.loop(0, YS)
        def _(y):
            d = planes[dz] + y
            for k in range(4):
                grad = g[d, k]
                momentum = hold_rate * m[d, k] + grad
                new_m[d, k] = momentum
                away[k // 2, d, pl.ds(4 * (k % 2), 4), :] = hold_rate * momentum + grad

    def send_away(c, dz):
        for d in partners(dz):
            send(away.at[c, d], there.at[c, me], away_send.at[c], away_recv.at[c], {"fsdp": d})

    def tell(n):
        for dz in (1, ZS - 1):
            pl.semaphore_signal(
                ready.at[n], inc=1, device_id={"fsdp": planes[dz] + own_y}, device_id_type=MESH
            )

    barrier = pltpu.get_barrier_semaphore()
    for dz in (1, ZS - 1, 0):
        for k in range(YS):
            if dz or k:
                pl.semaphore_signal(
                    barrier, inc=1, device_id={"fsdp": planes[dz] + ys[k]}, device_id_type=MESH
                )
    for k in range(1, 4):
        pl.semaphore_signal(barrier, inc=1, device_id={"tp": lax.rem(col + k, tp)}, device_id_type=MESH)

    for dz in OUTWARD:
        for copy in load(dz):
            copy.start()
    for dz in (1, ZS - 1, 0):
        direct(dz)

    pl.semaphore_wait(barrier, 3 * YS - 1 + tp - 1)
    tell(0)
    for c in range(2):
        for dz in (1, ZS - 1):
            send_away(c, dz)
        if c == 0:
            send_away(c, 0)
    for n in range(2):
        for dz in (n + 2, ZS - 2 - n):
            direct(dz)
        pl.semaphore_wait(ready.at[n], 2)
        tell(n + 1)
        for dz in (n + 2, ZS - 2 - n):
            send_away(0, dz)
    direct(4)
    pl.semaphore_wait(ready.at[2], 2)
    send_away(0, 4)
    for dz in (4, 5, 3, 6, 2, 0):
        send_away(1, dz)
    load_w = pltpu.make_async_copy(w_hbm, w, w_sem)
    load_w.start()
    for c in range(2):
        there[c, me] = away[c, me]

    @pl.loop(0, 2)
    def _(c):
        wait(there.at[c, pl.ds(0, fsdp - 1)], away_recv.at[c])

        @pl.loop(0, fsdp // 2)
        def _(j):
            first, second = swapped(there[c, 2 * j], there[c, 2 * j + 1])
            rows = pl.ds(pl.multiple_of(8 * j, 8), 8)
            mats[0, rows, :] = first
            mats[1, rows, :] = second

        for k in range(2):
            x = mats[k]
            gram[c, k] = dot(x, x, ((1,), (1,)))
        for k in range(1, 4):
            send(gram.at[c], grams.at[c, col], gram_send.at[c], gram_recv.at[c], {"tp": lax.rem(col + k, tp)})
        grams[c, col] = gram[c]
        wait(grams.at[c, pl.ds(0, tp - 1)], gram_recv.at[c])

        takens = iterated(
            [(grams[c, 0, k] + grams[c, 1, k]) + (grams[c, 2, k] + grams[c, 3, k]) for k in range(2)]
        )
        for k in range(2):
            mats[k] = dot(takens[k], mats[k])

        @pl.loop(0, fsdp // 2)
        def _(j):
            rows = pl.ds(pl.multiple_of(8 * j, 8), 8)
            first, second = swapped(mats[0, rows, :], mats[1, rows, :])
            home[c, 2 * j] = first
            home[c, 2 * j + 1] = second

        last = [planes[1] + own_y, planes[ZS - 1] + own_y]
        order = [d for dz in (0, 4, 5, 3, 6, 2) for d in partners_home(dz)]
        order += [d for pair in zip(partners_home(ZS - 1)[:3], partners_home(1)[:3]) for d in pair]
        for d in order + last:
            send(home.at[c, d], back.at[c, me], home_send.at[c], home_recv.at[c], {"fsdp": d})
        back[c, me] = home[c, me]

    load_w.wait()
    for c in range(2):
        wait(back.at[c, pl.ds(0, fsdp - 1)], home_recv.at[c])

        @pl.loop(0, fsdp)
        def _(d):
            for k in range(2):
                new_w[d, 2 * c + k] = (1.0 - learn_rate * decay_rate) * w[d, 2 * c + k] - learn_rate * back[
                    c, d, pl.ds(4 * k, 4), :
                ]

    for c in range(2):
        wait(away.at[c, pl.ds(0, fsdp - 1)], away_send.at[c])
        wait(home.at[c, pl.ds(0, fsdp - 1)], home_send.at[c])
        wait(grams.at[c, pl.ds(0, tp - 1)], gram_send.at[c])


def stored(a, b, a_out, b_out, sems):
    copies = [
        pltpu.make_async_copy(a, a_out, sems.at[0]),
        pltpu.make_async_copy(b, b_out, sems.at[1]),
    ]
    for copy in copies:
        copy.start()
    for copy in copies:
        copy.wait()


def shards(gradients, momentum, weights):
    mats, side, wide = gradients.shape
    fsdp = lax.axis_size("fsdp")
    tp = lax.axis_size("tp")
    shape = (fsdp, mats // fsdp, side, wide)
    rows = side * fsdp
    f32 = jnp.float32
    block = pltpu.VMEM(shape, f32)
    tiles = pltpu.VMEM((2, fsdp, 2 * side, wide), f32)
    sem = pltpu.SemaphoreType.DMA
    new_weights, new_momentum = pl.pallas_call(
        kernel,
        out_shape=[jax.ShapeDtypeStruct(shape, f32)] * 2,
        in_specs=[pl.BlockSpec(memory_space=pl.ANY)] * 3,
        out_specs=[pl.BlockSpec(memory_space=pltpu.VMEM)] * 2,
        scratch_shapes=[
            block, block, block, tiles, tiles, tiles, tiles,
            pltpu.VMEM((2, rows, wide), f32),
            pltpu.VMEM((2, 2, rows, rows), f32),
            pltpu.VMEM((2, tp, 2, rows, rows), f32),
            sem((ZS, 2)), sem, sem((2,)), sem((2,)), sem((2,)), sem((2,)), sem((2,)), sem((2,)),
            pltpu.SemaphoreType.REGULAR((3,)),
        ],
        compiler_params=pltpu.CompilerParams(
            collective_id=0, has_side_effects=True, vmem_limit_bytes=48 * 1024 * 1024
        ),
        name="update",
    )(gradients.reshape(shape), momentum.reshape(shape), weights.reshape(shape))
    new_weights, new_momentum = pl.pallas_call(
        stored,
        out_shape=[jax.ShapeDtypeStruct(shape, f32)] * 2,
        in_specs=[pl.BlockSpec(memory_space=pl.ANY)] * 2,
        out_specs=[pl.BlockSpec(memory_space=pl.ANY)] * 2,
        scratch_shapes=[sem((2,))],
        compiler_params=pltpu.CompilerParams(vmem_limit_bytes=1024 * 1024),
        name="stored",
    )(new_weights, new_momentum)
    return new_weights.reshape(gradients.shape), new_momentum.reshape(gradients.shape)


def solution(mesh):
    return jax.shard_map(
        shards,
        mesh=mesh,
        in_specs=(P("copy", "fsdp", "tp"), P("copy", "fsdp", "tp"), P("copy", "fsdp", "tp")),
        out_specs=(P("copy", "fsdp", "tp"), P("copy", "fsdp", "tp")),
        check_vma=False,
    )
```

```python
import jax
import jax.numpy as jnp
from jax import lax
from jax.experimental import pallas as pl
from jax.experimental.pallas import tpu as pltpu
from jax.sharding import PartitionSpec as P

ITERS = 4


hold_rate = 0.95
learn_rate = 0.9
decay_rate = 0.1

ZS, YS = 8, 4
OUTWARD = (1, 7, 0, 2, 6, 3, 5, 4)
MESH = pl.DeviceIdType.MESH
HIGHEST = lax.Precision.HIGHEST


def dot(a, b, contract=((1,), (0,))):
    return lax.dot_general(
        a, b, (contract, ((), ())), precision=HIGHEST, preferred_element_type=jnp.float32
    )


def send(src, dst, send_sem, recv_sem, device):
    pltpu.make_async_remote_copy(
        src_ref=src, dst_ref=dst, send_sem=send_sem, recv_sem=recv_sem, device_id=device, device_id_type=MESH
    ).start()


def wait(ref, sem):
    pltpu.make_async_copy(ref, ref, sem).wait()


def swapped(a, b):
    upper = lax.broadcasted_iota(jnp.int32, a.shape, 0) < 4
    return (
        jnp.where(upper, a, pltpu.roll(b, 4, 0)),
        jnp.where(upper, pltpu.roll(a, 4, 0), b),
    )


def iterated(grams):
    shape = grams[0].shape
    eye = (
        lax.broadcasted_iota(jnp.int32, shape, 0) == lax.broadcasted_iota(jnp.int32, shape, 1)
    ).astype(jnp.float32)
    scales = [
        lax.rsqrt(jnp.sum(jnp.sum(a * eye, axis=1, keepdims=True), axis=0, keepdims=True) + 1e-06)
        for a in grams
    ]
    grams = [a * (scale * scale) for a, scale in zip(grams, scales)]
    takens = None
    for step in range(ITERS):
        mixed = [3.4445 * eye - 4.775 * a + 2.0315 * dot(a, a) for a in grams]
        if step < ITERS - 1:
            halves = [dot(m, a) for m, a in zip(mixed, grams)]
        takens = mixed if takens is None else [dot(m, t) for m, t in zip(mixed, takens)]
        if step < ITERS - 1:
            grams = [dot(h, m) for h, m in zip(halves, mixed)]
    return [t * scale for t, scale in zip(takens, scales)]


def kernel(
    g_hbm, m_hbm, w_hbm, new_w, new_m,
    g, m, w, away, there, home, back, mats, gram, grams,
    load_sem, w_sem, away_send, away_recv, home_send, home_recv, gram_send, gram_recv, ready,
):
    fsdp = lax.axis_size("fsdp")
    tp = lax.axis_size("tp")
    me = lax.axis_index("fsdp")
    col = lax.axis_index("tp")
    core = lax.axis_index("copy")
    own_y = lax.rem(me, YS)
    planes = [lax.rem(me // YS + k, ZS) * YS for k in range(ZS)]
    ys = [lax.rem(own_y + k, YS) for k in range(YS)]
    shifted = [lax.rem(own_y + core + k, YS) for k in range(YS)]

    def partners(dz):
        if dz == 0:
            return [planes[0] + ys[k] for k in range(1, YS)]
        return [planes[dz] + shifted[(k + (2 if dz > ZS // 2 else 0)) % YS] for k in range(YS)]

    one, three = lax.rem(own_y + 1 + 2 * core, YS), lax.rem(own_y + 3 - 2 * core, YS)

    def partners_home(dz):
        if dz == 0:
            return partners(0)
        turn = [one, three] if dz <= ZS // 2 else [three, one]
        return [planes[dz] + y for y in (ys[2], *turn, ys[0])]

    def load(dz):
        rows = pl.ds(planes[dz], YS)
        return [
            pltpu.make_async_copy(x.at[rows], y.at[rows], load_sem.at[dz, n])
            for n, (x, y) in enumerate(((g_hbm, g), (m_hbm, m)))
        ]

    def direct(dz):
        for copy in load(dz):
            copy.wait()

        @pl.loop(0, YS)
        def _(y):
            d = planes[dz] + y
            for k in range(4):
                grad = g[d, k]
                momentum = hold_rate * m[d, k] + grad
                new_m[d, k] = momentum
                away[k // 2, d, pl.ds(4 * (k % 2), 4), :] = hold_rate * momentum + grad

    def send_away(c, dz):
        for d in partners_home(dz):
            send(away.at[c, d], there.at[c, me], away_send.at[c], away_recv.at[c], {"fsdp": d})

    def tell(n):
        for dz in (1, ZS - 1):
            pl.semaphore_signal(
                ready.at[n], inc=1, device_id={"fsdp": planes[dz] + own_y}, device_id_type=MESH
            )

    barrier = pltpu.get_barrier_semaphore()
    for dz in (1, ZS - 1, 0):
        for k in range(YS):
            if dz or k:
                pl.semaphore_signal(
                    barrier, inc=1, device_id={"fsdp": planes[dz] + ys[k]}, device_id_type=MESH
                )
    for k in range(1, 4):
        pl.semaphore_signal(barrier, inc=1, device_id={"tp": lax.rem(col + k, tp)}, device_id_type=MESH)

    for dz in OUTWARD:
        for copy in load(dz):
            copy.start()
    for dz in (1, ZS - 1, 0):
        direct(dz)

    pl.semaphore_wait(barrier, 3 * YS - 1 + tp - 1)
    tell(0)
    for c in range(2):
        for dz in (1, ZS - 1):
            send_away(c, dz)
        if c == 0:
            send_away(c, 0)
    for n in range(2):
        for dz in (n + 2, ZS - 2 - n):
            direct(dz)
        pl.semaphore_wait(ready.at[n], 2)
        tell(n + 1)
        for dz in (n + 2, ZS - 2 - n):
            send_away(0, dz)
    direct(4)
    pl.semaphore_wait(ready.at[2], 2)
    send_away(0, 4)
    for dz in (4, 5, 3, 6, 2, 0):
        send_away(1, dz)
    load_w = pltpu.make_async_copy(w_hbm, w, w_sem)
    load_w.start()
    for c in range(2):
        there[c, me] = away[c, me]

    @pl.loop(0, 2)
    def _(c):
        wait(there.at[c, pl.ds(0, fsdp - 1)], away_recv.at[c])

        @pl.loop(0, fsdp // 2)
        def _(j):
            first, second = swapped(there[c, 2 * j], there[c, 2 * j + 1])
            rows = pl.ds(pl.multiple_of(8 * j, 8), 8)
            mats[0, rows, :] = first
            mats[1, rows, :] = second

        for k in range(2):
            x = mats[k]
            gram[c, k] = dot(x, x, ((1,), (1,)))
        for k in range(1, 4):
            send(gram.at[c], grams.at[c, col], gram_send.at[c], gram_recv.at[c], {"tp": lax.rem(col + k, tp)})
        grams[c, col] = gram[c]
        wait(grams.at[c, pl.ds(0, tp - 1)], gram_recv.at[c])

        takens = iterated(
            [(grams[c, 0, k] + grams[c, 1, k]) + (grams[c, 2, k] + grams[c, 3, k]) for k in range(2)]
        )
        for k in range(2):
            mats[k] = dot(takens[k], mats[k])

        @pl.loop(0, fsdp // 2)
        def _(j):
            rows = pl.ds(pl.multiple_of(8 * j, 8), 8)
            first, second = swapped(mats[0, rows, :], mats[1, rows, :])
            home[c, 2 * j] = first
            home[c, 2 * j + 1] = second

        far = [d for dz in (0, 4, 5, 3, 6, 2) for d in partners_home(dz)]
        near = [d for pair in zip(partners_home(ZS - 1), partners_home(1)) for d in pair]
        for part, devices in enumerate((far, near)):
            for d in devices:
                send(home.at[c, d], back.at[c, me], home_send.at[c], home_recv.at[c, part], {"fsdp": d})
        back[c, me] = home[c, me]

    load_w.wait()
    def update(c, dz):
        @pl.loop(0, YS)
        def _(y):
            d = planes[dz] + y
            for k in range(2):
                new_w[d, 2 * c + k] = (1.0 - learn_rate * decay_rate) * w[d, 2 * c + k] - learn_rate * back[
                    c, d, pl.ds(4 * k, 4), :
                ]

    for c in range(2):
        for part, reached in enumerate(((0, 4, 5, 3, 6, 2), (ZS - 1, 1))):
            messages = YS * len(reached) - (1 - part)
            wait(back.at[c, pl.ds(0, messages)], home_recv.at[c, part])
            for dz in reached:
                update(c, dz)

    for c in range(2):
        wait(away.at[c, pl.ds(0, fsdp - 1)], away_send.at[c])
        wait(home.at[c, pl.ds(0, fsdp - 1)], home_send.at[c])
        wait(grams.at[c, pl.ds(0, tp - 1)], gram_send.at[c])


def stored(a, b, a_out, b_out, sems):
    copies = [
        pltpu.make_async_copy(a, a_out, sems.at[0]),
        pltpu.make_async_copy(b, b_out, sems.at[1]),
    ]
    for copy in copies:
        copy.start()
    for copy in copies:
        copy.wait()


def shards(gradients, momentum, weights):
    mats, side, wide = gradients.shape
    fsdp = lax.axis_size("fsdp")
    tp = lax.axis_size("tp")
    shape = (fsdp, mats // fsdp, side, wide)
    rows = side * fsdp
    f32 = jnp.float32
    block = pltpu.VMEM(shape, f32)
    tiles = pltpu.VMEM((2, fsdp, 2 * side, wide), f32)
    sem = pltpu.SemaphoreType.DMA
    new_weights, new_momentum = pl.pallas_call(
        kernel,
        out_shape=[jax.ShapeDtypeStruct(shape, f32)] * 2,
        in_specs=[pl.BlockSpec(memory_space=pl.ANY)] * 3,
        out_specs=[pl.BlockSpec(memory_space=pltpu.VMEM)] * 2,
        scratch_shapes=[
            block, block, block, tiles, tiles, tiles, tiles,
            pltpu.VMEM((2, rows, wide), f32),
            pltpu.VMEM((2, 2, rows, rows), f32),
            pltpu.VMEM((2, tp, 2, rows, rows), f32),
            sem((ZS, 2)), sem, sem((2,)), sem((2,)), sem((2,)), sem((2, 2)), sem((2,)), sem((2,)),
            pltpu.SemaphoreType.REGULAR((3,)),
        ],
        compiler_params=pltpu.CompilerParams(
            collective_id=0, has_side_effects=True, vmem_limit_bytes=48 * 1024 * 1024
        ),
        name="update",
    )(gradients.reshape(shape), momentum.reshape(shape), weights.reshape(shape))
    new_weights, new_momentum = pl.pallas_call(
        stored,
        out_shape=[jax.ShapeDtypeStruct(shape, f32)] * 2,
        in_specs=[pl.BlockSpec(memory_space=pl.ANY)] * 2,
        out_specs=[pl.BlockSpec(memory_space=pl.ANY)] * 2,
        scratch_shapes=[sem((2,))],
        compiler_params=pltpu.CompilerParams(vmem_limit_bytes=1024 * 1024),
        name="stored",
    )(new_weights, new_momentum)
    return new_weights.reshape(gradients.shape), new_momentum.reshape(gradients.shape)


def solution(mesh):
    return jax.shard_map(
        shards,
        mesh=mesh,
        in_specs=(P("copy", "fsdp", "tp"), P("copy", "fsdp", "tp"), P("copy", "fsdp", "tp")),
        out_specs=(P("copy", "fsdp", "tp"), P("copy", "fsdp", "tp")),
        check_vma=False,
    )
```

```python
import jax
import jax.numpy as jnp
from jax import lax
from jax.experimental import pallas as pl
from jax.experimental.pallas import tpu as pltpu
from jax.sharding import PartitionSpec as P

ITERS = 4


hold_rate = 0.95
learn_rate = 0.9
decay_rate = 0.1

ZS, YS = 8, 4
OUTWARD = (1, 7, 0, 2, 6, 3, 5, 4)
MESH = pl.DeviceIdType.MESH
HIGHEST = lax.Precision.HIGHEST


def dot(a, b, contract=((1,), (0,))):
    return lax.dot_general(
        a, b, (contract, ((), ())), precision=HIGHEST, preferred_element_type=jnp.float32
    )


def send(src, dst, send_sem, recv_sem, device):
    pltpu.make_async_remote_copy(
        src_ref=src, dst_ref=dst, send_sem=send_sem, recv_sem=recv_sem, device_id=device, device_id_type=MESH
    ).start()


def wait(ref, sem):
    pltpu.make_async_copy(ref, ref, sem).wait()


def swapped(a, b):
    upper = lax.broadcasted_iota(jnp.int32, a.shape, 0) < 4
    return (
        jnp.where(upper, a, pltpu.roll(b, 4, 0)),
        jnp.where(upper, pltpu.roll(a, 4, 0), b),
    )


def iterated(grams):
    shape = grams[0].shape
    eye = (
        lax.broadcasted_iota(jnp.int32, shape, 0) == lax.broadcasted_iota(jnp.int32, shape, 1)
    ).astype(jnp.float32)
    scales = [
        lax.rsqrt(jnp.sum(jnp.sum(a * eye, axis=1, keepdims=True), axis=0, keepdims=True) + 1e-06)
        for a in grams
    ]
    grams = [a * (scale * scale) for a, scale in zip(grams, scales)]
    takens = None
    for step in range(ITERS):
        mixed = [3.4445 * eye - 4.775 * a + 2.0315 * dot(a, a) for a in grams]
        if step < ITERS - 1:
            halves = [dot(m, a) for m, a in zip(mixed, grams)]
        takens = mixed if takens is None else [dot(m, t) for m, t in zip(mixed, takens)]
        if step < ITERS - 1:
            grams = [dot(h, m) for h, m in zip(halves, mixed)]
    return [t * scale for t, scale in zip(takens, scales)]


def kernel(
    g_hbm, m_hbm, w_hbm, new_w, new_m,
    g, m, w, away, there, home, back, mats, gram, grams,
    load_sem, w_sem, away_send, away_recv, home_send, home_recv, gram_send, gram_recv, ready,
):
    fsdp = lax.axis_size("fsdp")
    tp = lax.axis_size("tp")
    me = lax.axis_index("fsdp")
    col = lax.axis_index("tp")
    core = lax.axis_index("copy")
    own_y = lax.rem(me, YS)
    planes = [lax.rem(me // YS + k, ZS) * YS for k in range(ZS)]
    ys = [lax.rem(own_y + k, YS) for k in range(YS)]
    shifted = [lax.rem(own_y + core + k, YS) for k in range(YS)]

    def partners(dz):
        if dz == 0:
            return [planes[0] + ys[k] for k in range(1, YS)]
        return [planes[dz] + shifted[(k + (2 if dz > ZS // 2 else 0)) % YS] for k in range(YS)]

    one, three = lax.rem(own_y + 1 + 2 * core, YS), lax.rem(own_y + 3 - 2 * core, YS)

    def partners_home(dz):
        if dz == 0:
            return partners(0)
        turn = [one, three] if dz <= ZS // 2 else [three, one]
        return [planes[dz] + y for y in (ys[2], *turn, ys[0])]

    def load(dz):
        rows = pl.ds(planes[dz], YS)
        return [
            pltpu.make_async_copy(x.at[rows], y.at[rows], load_sem.at[dz, n])
            for n, (x, y) in enumerate(((g_hbm, g), (m_hbm, m)))
        ]

    def direct(dz):
        for copy in load(dz):
            copy.wait()

        @pl.loop(0, YS)
        def _(y):
            d = planes[dz] + y
            for k in range(4):
                grad = g[d, k]
                momentum = hold_rate * m[d, k] + grad
                new_m[d, k] = momentum
                away[k // 2, d, pl.ds(4 * (k % 2), 4), :] = hold_rate * momentum + grad

    def others(dz):
        turn = 2 if dz > ZS // 2 else 0
        return [planes[dz] + ys[1 + (k + turn) % 3] for k in range(3)]

    def send_away(c, dz, devices=None):
        for d in devices or partners_home(dz):
            send(away.at[c, d], there.at[c, me], away_send.at[c], away_recv.at[c], {"fsdp": d})

    def tell(n):
        for dz in (1, ZS - 1):
            pl.semaphore_signal(
                ready.at[n], inc=1, device_id={"fsdp": planes[dz] + own_y}, device_id_type=MESH
            )

    barrier = pltpu.get_barrier_semaphore()
    for d in (planes[1] + own_y, planes[ZS - 1] + own_y, *partners(0)):
        pl.semaphore_signal(barrier, inc=1, device_id={"fsdp": d}, device_id_type=MESH)
    for k in range(1, 4):
        pl.semaphore_signal(barrier, inc=1, device_id={"tp": lax.rem(col + k, tp)}, device_id_type=MESH)

    for dz in OUTWARD[:2]:
        for copy in load(dz):
            copy.start()

    pl.semaphore_wait(barrier, 2 + YS - 1 + tp - 1)
    tell(0)
    for dz in (1, ZS - 1):
        direct(dz)
        if dz == 1:
            for far in OUTWARD[2:]:
                for copy in load(far):
                    copy.start()
        for c in range(2):
            send_away(c, dz, [planes[dz] + own_y])
    pl.semaphore_wait(ready.at[0], 2)
    tell(1)
    for c in range(2):
        for dz in (1, ZS - 1):
            send_away(c, dz, others(dz))
    direct(0)
    send_away(0, 0)
    for n in (2, 3):
        pl.semaphore_wait(ready.at[n - 1], 2)
        tell(n)
        for dz in (n, ZS - n):
            direct(dz)
            send_away(0, dz)
    pl.semaphore_wait(ready.at[3], 2)
    direct(4)
    send_away(0, 4)
    for dz in (4, 5, 3, 6, 2, 0):
        send_away(1, dz)
    load_w = pltpu.make_async_copy(w_hbm, w, w_sem)
    load_w.start()
    for c in range(2):
        there[c, me] = away[c, me]

    @pl.loop(0, 2)
    def _(c):
        wait(there.at[c, pl.ds(0, fsdp - 1)], away_recv.at[c])

        @pl.loop(0, fsdp // 2)
        def _(j):
            first, second = swapped(there[c, 2 * j], there[c, 2 * j + 1])
            rows = pl.ds(pl.multiple_of(8 * j, 8), 8)
            mats[0, rows, :] = first
            mats[1, rows, :] = second

        for k in range(2):
            x = mats[k]
            gram[c, k] = dot(x, x, ((1,), (1,)))
        for k in range(1, 4):
            send(gram.at[c], grams.at[c, col], gram_send.at[c], gram_recv.at[c], {"tp": lax.rem(col + k, tp)})
        grams[c, col] = gram[c]
        wait(grams.at[c, pl.ds(0, tp - 1)], gram_recv.at[c])

        takens = iterated(
            [(grams[c, 0, k] + grams[c, 1, k]) + (grams[c, 2, k] + grams[c, 3, k]) for k in range(2)]
        )
        for k in range(2):
            mats[k] = dot(takens[k], mats[k])

        @pl.loop(0, fsdp // 2)
        def _(j):
            rows = pl.ds(pl.multiple_of(8 * j, 8), 8)
            first, second = swapped(mats[0, rows, :], mats[1, rows, :])
            home[c, 2 * j] = first
            home[c, 2 * j + 1] = second

        far = [d for dz in (0, 4, 5, 3, 6, 2) for d in partners_home(dz)]
        near = [d for pair in zip(partners_home(ZS - 1), partners_home(1)) for d in pair]
        for part, devices in enumerate((far, near)):
            for d in devices:
                send(home.at[c, d], back.at[c, me], home_send.at[c], home_recv.at[c, part], {"fsdp": d})
        back[c, me] = home[c, me]

    load_w.wait()
    def update(c, dz):
        @pl.loop(0, YS)
        def _(y):
            d = planes[dz] + y
            for k in range(2):
                new_w[d, 2 * c + k] = (1.0 - learn_rate * decay_rate) * w[d, 2 * c + k] - learn_rate * back[
                    c, d, pl.ds(4 * k, 4), :
                ]

    for c in range(2):
        for part, reached in enumerate(((0, 4, 5, 3, 6, 2), (ZS - 1, 1))):
            messages = YS * len(reached) - (1 - part)
            wait(back.at[c, pl.ds(0, messages)], home_recv.at[c, part])
            for dz in reached:
                update(c, dz)

    for c in range(2):
        wait(away.at[c, pl.ds(0, fsdp - 1)], away_send.at[c])
        wait(home.at[c, pl.ds(0, fsdp - 1)], home_send.at[c])
        wait(grams.at[c, pl.ds(0, tp - 1)], gram_send.at[c])


def stored(a, b, a_out, b_out, sems):
    copies = [
        pltpu.make_async_copy(a, a_out, sems.at[0]),
        pltpu.make_async_copy(b, b_out, sems.at[1]),
    ]
    for copy in copies:
        copy.start()
    for copy in copies:
        copy.wait()


def shards(gradients, momentum, weights):
    mats, side, wide = gradients.shape
    fsdp = lax.axis_size("fsdp")
    tp = lax.axis_size("tp")
    shape = (fsdp, mats // fsdp, side, wide)
    rows = side * fsdp
    f32 = jnp.float32
    block = pltpu.VMEM(shape, f32)
    tiles = pltpu.VMEM((2, fsdp, 2 * side, wide), f32)
    sem = pltpu.SemaphoreType.DMA
    new_weights, new_momentum = pl.pallas_call(
        kernel,
        out_shape=[jax.ShapeDtypeStruct(shape, f32)] * 2,
        in_specs=[pl.BlockSpec(memory_space=pl.ANY)] * 3,
        out_specs=[pl.BlockSpec(memory_space=pltpu.VMEM)] * 2,
        scratch_shapes=[
            block, block, block, tiles, tiles, tiles, tiles,
            pltpu.VMEM((2, rows, wide), f32),
            pltpu.VMEM((2, 2, rows, rows), f32),
            pltpu.VMEM((2, tp, 2, rows, rows), f32),
            sem((ZS, 2)), sem, sem((2,)), sem((2,)), sem((2,)), sem((2, 2)), sem((2,)), sem((2,)),
            pltpu.SemaphoreType.REGULAR((4,)),
        ],
        compiler_params=pltpu.CompilerParams(
            collective_id=0, has_side_effects=True, vmem_limit_bytes=48 * 1024 * 1024
        ),
        name="update",
    )(gradients.reshape(shape), momentum.reshape(shape), weights.reshape(shape))
    new_weights, new_momentum = pl.pallas_call(
        stored,
        out_shape=[jax.ShapeDtypeStruct(shape, f32)] * 2,
        in_specs=[pl.BlockSpec(memory_space=pl.ANY)] * 2,
        out_specs=[pl.BlockSpec(memory_space=pl.ANY)] * 2,
        scratch_shapes=[sem((2,))],
        compiler_params=pltpu.CompilerParams(vmem_limit_bytes=1024 * 1024),
        name="stored",
    )(new_weights, new_momentum)
    return new_weights.reshape(gradients.shape), new_momentum.reshape(gradients.shape)


def solution(mesh):
    return jax.shard_map(
        shards,
        mesh=mesh,
        in_specs=(P("copy", "fsdp", "tp"), P("copy", "fsdp", "tp"), P("copy", "fsdp", "tp")),
        out_specs=(P("copy", "fsdp", "tp"), P("copy", "fsdp", "tp")),
        check_vma=False,
    )
```
